256 devices in a mesh: gx: 4 (over y), gy: 8 (over x, core), gz: 8 (over z).
Axes of the slice: x: 4, y: 4, z: 8, core: 2. Of those that a mesh axis runs over, the one named last changes fastest.
Arguments:
- start_block: float32 [64, 3, 8, 64, 1024], P(None, None, 'gx', 'gy', 'gz'), may hold values from -6 to 6
- stiff_field: float32 [8, 64, 1024], P('gx', 'gy', 'gz'), may hold values from 0.5 to 2
- shift_field: float32 [8, 64, 1024], P('gx', 'gy', 'gz'), may hold values from 0.25 to 2
- mass_field: float32 [8, 64, 1024], P('gx', 'gy', 'gz'), may hold values from 0.5 to 2
Outputs:
- modes: float32 [64, 3, 8, 64, 1024], P(None, None, 'gx', 'gy', 'gz')
- ritz: float32 [64, 64], replicated
The draws below stay inside these ranges and needn't reach their ends.
All inputs are finite; a program needn't handle non-finite values. Where the reference program divides by a largest or mean magnitude, that divisor is 1e-20 or more.
Results may differ from the reference program's by a relative error of at most 0.0003.
Values sent between devices are 32-bit elements; how exact they have to be, the bound alone decides.
A program may use at most 128 MiB of HBM per device.

```python
import math
import jax
import jax.numpy as jnp
from jax import lax

MODES = 64
ITERS = 2
FILTER = 4
NX = 8
NY = 64
NZ = 1024
DOFS = 1572864


def steps_of(rng, shape, cuts, smallest, top_value):
    def one(axis_at, parts):
        steps = jax.random.uniform(jax.random.fold_in(jax.random.fold_in(rng, 6), axis_at), (parts,), jnp.float32, smallest / len(cuts), top_value / len(cuts))
        return jnp.repeat(jnp.exp(steps), shape[axis_at] // parts).reshape((-1,) + (1,) * (len(shape) - axis_at - 1))

    gain = one(*cuts[0])
    for cut in cuts[1:]:
        gain = gain * one(*cut)
    return gain


def noise(key, shape, scale, limit, cuts=(), dtype=jnp.bfloat16):
    result = jax.random.normal(key, shape, jnp.float32) * scale
    if len(cuts) > 0:
        result = steps_of(key, shape, cuts, -0.22, 0.18) * result
    return jnp.clip(result, min=-limit, max=limit).astype(dtype)


def setup_inputs(seed: int = 0) -> dict:
    seeds = jax.random.split(jax.random.key(seed), 5)
    start_block = noise(seeds[0], (MODES, 3, NX, NY, NZ), 1.0, 6.0, ((2, 4), (3, 8), (4, 8)), jnp.float32)
    stiff_field = jnp.clip(jnp.exp(math.log(2.0) - 1.3862944 * jax.random.uniform(seeds[1], (NX, NY, NZ), jnp.float32) ** steps_of(seeds[1], (NX, NY, NZ), ((0, 4), (1, 8), (2, 8)), -0.2, 0.2)), 0.5, 2.0)
    shift_field = jnp.clip(jnp.exp(math.log(2.0) - 2.0794415 * jax.random.uniform(seeds[2], (NX, NY, NZ), jnp.float32) ** steps_of(seeds[2], (NX, NY, NZ), ((0, 4), (1, 8), (2, 8)), -0.2, 0.2)), 0.25, 2.0)
    mass_field = jnp.clip(jnp.exp(math.log(2.0) - 1.3862944 * jax.random.uniform(seeds[3], (NX, NY, NZ), jnp.float32) ** steps_of(seeds[3], (NX, NY, NZ), ((0, 4), (1, 8), (2, 8)), -0.2, 0.2)), 0.5, 2.0)
    return {"start_block": start_block, "stiff_field": stiff_field, "shift_field": shift_field, "mass_field": mass_field}


def lower_solve(lower_mat, rhs):
    return lax.linalg.triangular_solve(lower_mat, rhs, left_side=True, lower=True)

def lower_trans_solve(lower_mat, rhs):
    return lax.linalg.triangular_solve(lower_mat, rhs, left_side=True, lower=True, transpose_a=True)

def hidot(left, right):
    return jnp.dot(left.astype(jnp.float32), right.astype(jnp.float32), precision=lax.Precision.HIGHEST, preferred_element_type=jnp.float32)

def gram_of(left, right):
    return hidot(left.reshape(left.shape[0], -1), right.reshape(right.shape[0], -1).T)

def combine(coeffs, vectors):
    flat = hidot(coeffs.T, vectors.reshape(vectors.shape[0], -1))
    return flat.reshape((coeffs.shape[1],) + vectors.shape[1:])

def stiffness(field, stiff_field, shift_field):
    scaled = stiff_field * field
    padded = jnp.pad(scaled, ((0, 0), (0, 0), (1, 1), (1, 1), (1, 1)))
    beside_all = padded[:, :, 2:, 1:-1, 1:-1] + padded[:, :, :-2, 1:-1, 1:-1]
    beside_all = beside_all + padded[:, :, 1:-1, 2:, 1:-1] + padded[:, :, 1:-1, :-2, 1:-1]
    beside_all = beside_all + padded[:, :, 1:-1, 1:-1, 2:] + padded[:, :, 1:-1, 1:-1, :-2]
    laplace = 6.0 * scaled - beside_all
    summed = jnp.sum(field, axis=1, keepdims=True)
    return stiff_field * laplace + shift_field * (field + 0.5 * summed)

def ritz_filter(pencil_k, pencil_m, mode_count):
    factor = jnp.linalg.cholesky(pencil_m)
    partial_value = lower_solve(factor, pencil_k)
    reduced = lower_solve(factor, partial_value.T).T
    gershgorin = jnp.max(jnp.sum(jnp.abs(reduced), axis=1))
    search = factor.T[:, :mode_count]
    for sweep_index in range(FILTER):
        search = search - hidot(reduced, search) / gershgorin
    correlation = hidot(search.T, search)
    small_factor = jnp.linalg.cholesky(correlation)
    orthonormal = lower_solve(small_factor, search.T).T
    coeffs = lower_trans_solve(factor, orthonormal)
    ritz_matrix = hidot(orthonormal.T, hidot(reduced, orthonormal))
    return (coeffs, ritz_matrix)

def reference(start_block, stiff_field, shift_field, mass_field):
    count = MODES
    start_image = stiffness(start_block, stiff_field, shift_field)
    mass_gram = gram_of(start_block, mass_field * start_block) / DOFS
    stiff_gram = gram_of(start_block, start_image) / DOFS
    factor = jnp.linalg.cholesky(mass_gram)
    current = lower_solve(factor, start_block.reshape(count, -1)).reshape(start_block.shape)
    stiff_image = lower_solve(factor, start_image.reshape(count, -1)).reshape(start_block.shape)
    ritz_matrix = lower_solve(factor, lower_solve(factor, stiff_gram).T).T
    diagonal = 6.0 * stiff_field * stiff_field + 1.5 * shift_field
    previous = None
    for iteration in range(ITERS):
        residual = (stiff_image - mass_field * combine(ritz_matrix, current)) / diagonal
        stiff_resid = stiffness(residual, stiff_field, shift_field)
        if iteration == 0:
            search_set = jnp.concatenate([current, residual], axis=0)
            image_set = jnp.concatenate([stiff_image, stiff_resid], axis=0)
        else:
            search_set = jnp.concatenate([current, residual, previous[0]], axis=0)
            image_set = jnp.concatenate([stiff_image, stiff_resid, previous[1]], axis=0)
        pencil_k = gram_of(search_set, image_set) / DOFS
        pencil_m = gram_of(search_set, mass_field * search_set) / DOFS
        coeffs, ritz_matrix = ritz_filter(pencil_k, pencil_m, count)
        current = combine(coeffs, search_set)
        stiff_image = combine(coeffs, image_set)
        previous = (combine(coeffs[count:], search_set[count:]), combine(coeffs[count:], image_set[count:]))
    return (current, ritz_matrix)
```

```python
import functools

import jax
import jax.numpy as jnp
from jax import lax
from jax.experimental import pallas as pl
from jax.experimental.pallas import tpu as pltpu
from jax.sharding import PartitionSpec as P

MESH = pl.DeviceIdType.MESH
F32 = jnp.float32
NV = 64
T = 128
NX, NC, NY = 2, 3, 8
PLANE = NC * NY * T
COLS = NX * PLANE
EDGE = NX * NC * T
X_LO, X_HI = 0, PLANE
Y_LO, Y_HI = 2 * PLANE, 2 * PLANE + EDGE
Z_AT = 2 * PLANE + 2 * EDGE
HALO = Z_AT + T
CH = NY * T
FAR_FIRST = {4: (2, 1, 3), 8: (4, 3, 5, 2, 6, 1, 7)}


def mm(a, b, ca=1, cb=0):
    return lax.dot_general(
        a, b, (((ca,), (cb,)), ((), ())), precision=lax.Precision.HIGHEST, preferred_element_type=F32
    )


def nt(a, b):
    return mm(a, b, 1, 1)


def tn(a, b):
    return mm(a, b, 0, 0)


def eye(n):
    return jnp.where(
        lax.broadcasted_iota(jnp.int32, (n, n), 0) == lax.broadcasted_iota(jnp.int32, (n, n), 1), 1.0, 0.0
    ).astype(F32)


def factor_inverse(a):
    n, p = NV, 8
    m = jnp.concatenate([a, eye(n)], axis=1)

    def full(x):
        return jnp.broadcast_to(x, (8, 2 * n))

    rows = [m[8 * i : 8 * i + 8, :] for i in range(n // 8)]
    sub = lax.broadcasted_iota(jnp.int32, (8, 2 * n), 0)
    pivots = []
    for v in range(n // 8):
        k = v * 8
        col = [{i: full(rows[i][:, k + t : k + t + 1]) for i in range(v, 8)} for t in range(p)]
        blk = [[full(col[u][v][t : t + 1, :]) if u <= t else None for u in range(p)] for t in range(p)]
        row = [full(rows[v][t : t + 1, :]) for t in range(p)]
        fac, piv = [None] * p, [None] * p
        for a_ in range(0, p, 2):
            b_ = a_ + 1
            i0 = 1.0 / blk[a_][a_]
            det = blk[a_][a_] * blk[b_][b_] - blk[b_][a_] * blk[b_][a_]
            i1 = blk[a_][a_] * (1.0 / det)
            low = blk[b_][a_] * i0
            piv[a_] = blk[a_][a_]
            piv[b_] = blk[b_][b_] - low * blk[b_][a_]
            row[b_] = row[b_] - low * row[a_]
            f0 = {i: col[a_][i] * i0 for i in range(v, 8)}
            f1 = {i: (col[b_][i] - col[a_][i] * low) * i1 for i in range(v, 8)}
            fac[a_], fac[b_] = f0, f1
            h0, g1, h1 = {}, {}, {}
            for t in range(b_ + 1, p):
                h0[t] = blk[t][a_] * i0
                g1[t] = blk[t][b_] - h0[t] * blk[b_][a_]
                h1[t] = g1[t] * i1
            for t in range(b_ + 1, p):
                for u in range(b_ + 1, t + 1):
                    blk[t][u] = blk[t][u] - h0[t] * blk[u][a_] - h1[t] * g1[u]
                row[t] = row[t] - h0[t] * row[a_] - h1[t] * row[b_]
                for i in range(v, 8):
                    col[t][i] = col[t][i] - f0[i] * blk[t][a_] - f1[i] * g1[t]
        d = piv[0]
        for t in range(1, p):
            d = jnp.where(sub >= t, piv[t], d)
        pivots.append(d)
        for i in range(v, 8):
            acc = None
            for t in range(p):
                if i == v and t == 7:
                    continue
                f = fac[t][i]
                if i == v:
                    f = jnp.where(sub > t, f, 0.0)
                acc = f * row[t] if acc is None else acc + f * row[t]
            rows[i] = rows[i] - acc
    return jnp.concatenate([r * lax.rsqrt(d) for r, d in zip(rows, pivots)], axis=0)[:, n:]


def filtered(h):
    n = h.shape[0]
    bound = jnp.max(jnp.sum(jnp.abs(h), axis=1, keepdims=True), axis=0, keepdims=True)
    f = eye(n) - h / bound
    f2 = mm(f, f)
    y = mm(f2, f2[:, :NV])
    qt = nt(factor_inverse(tn(y, y)), y)
    th = mm(qt, h)
    return qt, th, nt(th, qt)


def kernel(
    dofs, sizes,
    s, g, e, rho, out, ritz,
    V, KV, H, BR, OB, HB, HS, QF, QX, QH, YP, YK, YR, ZK, ZR, CO,
    P0, P1, P2, A0, A1, A2, B0, B1, B2, C0, C1, C2, D0, D1, D2,
    SM, ar_sem, halo_sem,
):
    me = {a: lax.axis_index(a) for a in ("gx", "gy", "gz")}
    lane = lax.broadcasted_iota(jnp.int32, (8, T), 1)

    def peer(axis, off):
        return lax.rem(me[axis] + off, sizes[axis])

    barrier = pltpu.get_barrier_semaphore()
    zero, one = jnp.zeros((NV, NV), F32), eye(NV)
    for axis in ("gx", "gy", "gz"):
        for off in FAR_FIRST[sizes[axis]]:
            pl.semaphore_signal(barrier, inc=1, device_id={axis: peer(axis, off)}, device_id_type=MESH)

    def remote(src, dst, send, recv, axis, to):
        return pltpu.make_async_remote_copy(
            src_ref=src, dst_ref=dst, send_sem=send, recv_sem=recv, device_id={axis: to}, device_id_type=MESH
        )

    def tile(k):
        return slice(k * T, (k + 1) * T)

    def at(x, c, y):
        return (x * NC + c) * NY + y

    def block(start, n=8):
        return pl.ds(pl.multiple_of(start, 8), n)

    diag = 6.0 * g[...] * g[...] + 1.5 * e[...]
    inv = 1.0 / diag
    CO[0] = inv
    CO[1] = rho[...] * inv
    CO[2] = g[...] * inv

    def load(b, _):
        up, down = jnp.zeros((8, T), F32), jnp.zeros((8, T), F32)
        rows = block(b * 8)
        for x in range(NX):
            for y in range(NY):
                r = x * NY + y
                gr, qr, mr = g[r : r + 1, :], CO[1, r : r + 1, :], rho[r : r + 1, :]
                for c in range(NC):
                    k = at(x, c, y)
                    v = s[pl.ds(b * 384 + (c * NX + x) * NY + y, 8, stride=48), :]
                    h = gr * v
                    V[rows, tile(k)] = v
                    H[rows, tile(k)] = h
                    BR[rows, tile(k)] = mr * v
                    OB[block(NV + b * 8), tile(k)] = qr * v
                    if y == NY - 1:
                        YK[0, rows, tile(x * NC + c)] = h
                    if y == 0:
                        YK[1, rows, tile(x * NC + c)] = h
                    up = jnp.where(lane == 2 * k, pltpu.roll(h, (2 * k + 1) % T, 1), up)
                    down = jnp.where(lane == (2 * k - 1) % T, pltpu.roll(h, (2 * k - 1) % T, 1), down)
        ZK[0, rows, :] = up
        ZK[1, rows, :] = down
        return 0

    lax.fori_loop(0, NV // 8, load, 0)
    up, down = jnp.zeros((8, T), F32), jnp.zeros((8, T), F32)
    for x in range(NX):
        for y in range(NY):
            q = jnp.broadcast_to(CO[1, x * NY + y : x * NY + y + 1, :], (8, T))
            QF[:, tile(x * NY + y)] = q
            for c in range(NC):
                k = at(x, c, y)
                if y == NY - 1:
                    YK[0, NV : NV + 8, tile(x * NC + c)] = q
                if y == 0:
                    YK[1, NV : NV + 8, tile(x * NC + c)] = q
                up = jnp.where(lane == 2 * k, pltpu.roll(q, (2 * k + 1) % T, 1), up)
                down = jnp.where(lane == (2 * k - 1) % T, pltpu.roll(q, (2 * k - 1) % T, 1), down)
    ZK[0, NV : NV + 8, :] = up
    ZK[1, NV : NV + 8, :] = down

    pl.semaphore_wait(barrier, sum(sizes.values()) - 3)

    all_rows = pl.ds(0, NV)

    def exchange(n, faces):
        started, arrived = [], []
        for i, (axis, up_src, down_src, low, high) in enumerate(faces):
            here, size = me[axis], sizes[axis]
            up_copy = remote(
                up_src, low, halo_sem.at[n, 0, 2 * i], halo_sem.at[n, 1, 2 * i], axis, lax.rem(here + 1, size)
            )
            down_copy = remote(
                down_src, high, halo_sem.at[n, 0, 2 * i + 1], halo_sem.at[n, 1, 2 * i + 1],
                axis, lax.rem(here + size - 1, size),
            )
            started += [(here < size - 1, up_copy), (here > 0, down_copy)]
            arrived += [(here > 0, up_copy, low), (here < size - 1, down_copy, high)]

        def start():
            for cond, copy in started:
                pl.when(cond)(copy.start)

        def wait():
            for cond, copy, place in arrived:
                pl.when(cond)(copy.wait_recv)

                @pl.when(jnp.logical_not(cond))
                def _():
                    place[...] = jnp.zeros(place.shape, F32)

        def finish():
            for cond, copy in started:
                pl.when(cond)(copy.wait_send)

        return start, wait, finish

    first = exchange(0, [
        ("gx", H.at[:, PLANE:COLS], H.at[:, 0:PLANE], HS.at[0, :, X_LO : X_LO + PLANE], HS.at[0, :, X_HI : X_HI + PLANE]),
        ("gx", QF.at[:, CH : 2 * CH], QF.at[:, 0:CH], QX.at[0], QX.at[1]),
        ("gy", YK.at[0], YK.at[1], YR.at[0], YR.at[1]),
        ("gz", ZK.at[0], ZK.at[1], ZR.at[0, 0], ZR.at[0, 1]),
    ])

    def later(n):
        top = 2 * NV * (n - 1)
        row = pl.ds(top, NV)
        return exchange(n, [
            ("gz", ZK.at[2 * n, 0:NV], ZK.at[2 * n + 1, 0:NV], ZR.at[n, 0, 0:NV], ZR.at[n, 1, 0:NV]),
            ("gy", YK.at[2 * n, 0:NV], YK.at[2 * n + 1, 0:NV], HB.at[row, Y_LO : Y_LO + EDGE], HB.at[row, Y_HI : Y_HI + EDGE]),
            ("gx", YP.at[n - 1, :, PLANE:COLS], YP.at[n - 1, :, 0:PLANE], HB.at[row, X_LO : X_LO + PLANE], HB.at[row, X_HI : X_HI + PLANE]),
        ])

    def stiffness(n, again):
        row = n * NV

        def body(b, _):
            up, down = jnp.zeros((8, T), F32), jnp.zeros((8, T), F32)
            rows, full = block(b * 8), block(row + b * 8)
            ends = HS[n % 2, rows, Z_AT:HALO]
            for x in range(NX):
                for y in range(NY):
                    r = x * NY + y
                    gr, er = g[r : r + 1, :], e[r : r + 1, :]
                    vs = [V[full, tile(at(x, c, y))] for c in range(NC)]
                    half = 0.5 * (vs[0] + vs[1] + vs[2])
                    for c in range(NC):
                        k = at(x, c, y)
                        h = H[rows, tile(k)]
                        face = HS[n % 2, rows, X_LO * (1 - x) + X_HI * x + (c * NY + y) * T : X_LO * (1 - x) + X_HI * x + (c * NY + y + 1) * T]
                        near = H[rows, tile(at(1 - x, c, y))] + face
                        y_at = (x * NC + c) * T
                        if y == 0:
                            near = near + HS[n % 2, rows, Y_LO + y_at : Y_LO + y_at + T]
                        else:
                            near = near + H[rows, tile(k - 1)]
                        if y == NY - 1:
                            near = near + HS[n % 2, rows, Y_HI + y_at : Y_HI + y_at + T]
                        else:
                            near = near + H[rows, tile(k + 1)]
                        end = pltpu.roll(ends, (-2 * k) % T, 1) if k else ends
                        near = near + jnp.where(lane == 0, end, pltpu.roll(h, 1, 1))
                        near = near + jnp.where(lane == T - 1, end, pltpu.roll(h, T - 1, 1))
                        kv = gr * (6.0 * h - near) + er * (vs[c] + half)
                        KV[full, tile(k)] = kv
                        if again:
                            OB[block(2 * row + b * 8), tile(k)] = CO[0, r : r + 1, :] * kv
                            w = CO[2, r : r + 1, :] * kv
                            YP[n, rows, tile(k)] = w
                            if y == NY - 1:
                                YK[2 * n + 2, rows, tile(x * NC + c)] = w
                            if y == 0:
                                YK[2 * n + 3, rows, tile(x * NC + c)] = w
                            up = jnp.where(lane == 2 * k, pltpu.roll(w, (2 * k + 1) % T, 1), up)
                            down = jnp.where(lane == (2 * k - 1) % T, pltpu.roll(w, (2 * k - 1) % T, 1), down)
            if again:
                ZK[2 * n + 2, rows, :] = up
                ZK[2 * n + 3, rows, :] = down
            return 0

        lax.fori_loop(0, NV // 8, body, 0)

    def grams(n, part):
        rows = NV * (n + 1)

        def body(j, acc):
            cols = pl.ds(pl.multiple_of(j * CH, CH), CH)
            left = acc[0] + nt(V[0:rows, cols], BR[:, cols])
            return left, acc[1] + nt(KV[0:rows, cols], V[n * NV : rows, cols])

        zero = jnp.zeros((rows, NV), F32)
        left, right = lax.fori_loop(0, COLS // CH, body, (zero, zero))
        part[...] = jnp.concatenate([left, right], axis=1).reshape(part.shape)

    def all_reduce(n, part, a, b, c, d, then):
        def spread(phase, axis, source, place):
            here = me[axis]
            copies = []
            for off in FAR_FIRST[sizes[axis]]:
                to = peer(axis, off)
                copy = remote(source(to), place.at[here], ar_sem.at[n, 0, phase, off], ar_sem.at[n, 1, phase, here], axis, to)
                copy.start()
                copies.append(copy)
            return copies

        def collect(phase, axis, place):
            for off in FAR_FIRST[sizes[axis]]:
                frm = peer(axis, off)
                remote(place.at[frm], place.at[frm], ar_sem.at[n, 0, phase, off], ar_sem.at[n, 1, phase, frm], axis, frm).wait_recv()

        def total(place):
            acc = place[0]
            for i in range(1, place.shape[0]):
                acc = acc + place[i]
            return acc

        copies = spread(0, "gy", lambda to: part.at[to], a)
        a[me["gy"]] = part[me["gy"]]
        collect(0, "gy", a)
        b[me["gx"]] = total(a)
        copies += spread(1, "gx", lambda to: b.at[me["gx"]], b)
        collect(1, "gx", b)
        c[me["gz"]] = total(b)
        copies += spread(2, "gz", lambda to: c.at[me["gz"]], c)
        then()
        collect(2, "gz", c)
        d[me["gy"]] = total(c)
        copies += spread(3, "gy", lambda to: d.at[me["gy"]], d)
        collect(3, "gy", d)
        for copy in copies:
            copy.wait_send()
        return d[...].reshape(-1, T) * (1.0 / dofs)

    def residual(n, coeffs):
        depth = 2 * NV * n
        last = n == 2

        def body(j, _):
            cols = pl.ds(pl.multiple_of(j * CH, CH), CH)
            r = mm(coeffs, OB[0:depth, cols])
            V[n * NV : (n + 1) * NV, cols] = r
            x8 = lax.div(j, NC) * NY
            for y in range(NY):
                part = r[:, tile(y)]
                row = pl.ds(x8 + y, 1)
                here = pl.ds(pl.multiple_of(j * CH + y * T, T), T)
                H[:, here] = g[row, :] * part
                BR[:, here] = rho[row, :] * part
                if not last:
                    OB[depth + NV : depth + 2 * NV, here] = CO[1, row, :] * part
            return 0

        lax.fori_loop(0, COLS // CH, body, 0)

    def residual_halo(n, coeffs):
        depth = 2 * NV * n
        last = n == 2

        def put(cols, q):
            r = mm(coeffs, HB[0:depth, cols])
            HS[n % 2, :, cols] = r
            if not last:
                HB[depth + NV : depth + 2 * NV, cols] = jnp.concatenate([q] * (NV // 8), axis=0) * r

        def body(j, _):
            cols = pl.ds(pl.multiple_of(j * CH, CH), CH)
            put(cols, QH[:, cols])
            return 0

        lax.fori_loop(0, 2 * NC, body, 0)
        put(slice(Y_LO, HALO), QH[:, Y_LO:HALO])

    first[0]()
    first[1]()
    for i, at_x in enumerate((X_LO, X_HI)):
        for c in range(NC):
            QH[:, at_x + c * CH : at_x + (c + 1) * CH] = QX[i]
    for i, at_y in enumerate((Y_LO, Y_HI)):
        HS[0, :, at_y : at_y + EDGE] = YR[i, 0:NV, :]
        QH[:, at_y : at_y + EDGE] = YR[i, NV : NV + 8, :]
    HS[0, :, Z_AT:HALO] = ZR[0, 0, 0:NV, :] + ZR[0, 1, 0:NV, :]
    QH[:, Z_AT:HALO] = ZR[0, 0, NV : NV + 8, :] + ZR[0, 1, NV : NV + 8, :]
    stiffness(0, True)
    grams(0, P0)
    second, third = later(1), later(2)

    def during_first():
        second[0]()
        first[2]()

        def body(b, _):
            for k in range(HALO // T):
                HB[block(NV + b * 8), tile(k)] = QH[:, tile(k)] * HS[0, block(b * 8), tile(k)]
            return 0

        lax.fori_loop(0, NV // 8, body, 0)

    G = all_reduce(0, P0, A0, B0, C0, D0, during_first)
    li0 = factor_inverse(G[:, :NV])
    theta0 = nt(mm(li0, G[:, NV:]), li0)
    c0 = jnp.concatenate([li0, -mm(theta0, li0)], axis=1)
    SM[0], SM[1] = li0, theta0
    residual(1, c0)
    second[1]()
    HB[0:NV, Z_AT:HALO] = ZR[1, 0, 0:NV, :] + ZR[1, 1, 0:NV, :]
    residual_halo(1, c0)
    stiffness(1, True)
    grams(1, P1)

    G = all_reduce(1, P1, A1, B1, C1, D1, third[0])
    li0, theta0 = SM[0], SM[1]
    cross = mm(li0, G[:NV, :])
    mxr, kxr = cross[:, :NV], cross[:, NV:]
    li_r = factor_inverse(G[NV:, :NV] - tn(mxr, mxr))
    li = jnp.concatenate(
        [jnp.concatenate([one, zero], axis=1), jnp.concatenate([-nt(li_r, mxr), li_r], axis=1)], axis=0
    )
    ga = jnp.concatenate(
        [jnp.concatenate([theta0, kxr], axis=1), jnp.concatenate([kxr.T, G[NV:, NV:]], axis=1)], axis=0
    )
    h = nt(mm(li, ga), li)
    qt, th, theta1 = filtered(h)
    ct = mm(qt, li)
    a2t = ct[:, NV:]
    a1t = mm(ct[:, :NV], li0)
    c1 = jnp.concatenate([a1t, -mm(theta1, a1t), a2t, -mm(theta1, a2t)], axis=1)
    ut = jnp.concatenate([nt(a2t, mxr), qt[:, NV:]], axis=1)
    SM[2], SM[3], SM[4] = theta1, a1t, a2t
    mxp, mpp = nt(qt, ut), nt(ut, ut)
    SM[5], SM[6], SM[7], SM[8] = mxp, mpp - tn(mxp, mxp), nt(th, ut), nt(mm(ut, h), ut)
    residual(2, c1)
    third[1]()
    HB[2 * NV : 3 * NV, Z_AT:HALO] = ZR[2, 0, 0:NV, :] + ZR[2, 1, 0:NV, :]
    residual_halo(2, c1)
    stiffness(2, False)
    grams(2, P2)

    G = all_reduce(2, P2, A2, B2, C2, D2, lambda: None)
    theta1, a1t, a2t, mxp, spp, kxp, kpp = (SM[i] for i in range(2, 9))
    cross_p = mm(a2t, G[NV : 2 * NV, :])
    cross = mm(jnp.concatenate([a1t, a2t], axis=1), G[: 2 * NV, :])
    mxr, kxr = cross[:, :NV], cross[:, NV:]
    mpr, kpr = cross_p[:, :NV], cross_p[:, NV:]
    li_r = factor_inverse(G[2 * NV :, :NV] - tn(mxr, mxr))
    l32 = nt(mpr - tn(mxp, mxr), li_r)
    li_p = factor_inverse(spp - nt(l32, l32))
    below = -nt(li_r, mxr)
    li = jnp.concatenate(
        [
            jnp.concatenate([one, zero, zero], axis=1),
            jnp.concatenate([below, li_r, zero], axis=1),
            jnp.concatenate([mm(li_p, -mxp.T - mm(l32, below)), -mm(li_p, mm(l32, li_r)), li_p], axis=1),
        ],
        axis=0,
    )
    ga = jnp.concatenate(
        [
            jnp.concatenate([theta1, kxr, kxp], axis=1),
            jnp.concatenate([kxr.T, G[2 * NV :, NV:], kpr.T], axis=1),
            jnp.concatenate([kxp.T, kpr, kpp], axis=1),
        ],
        axis=0,
    )
    h = nt(mm(li, ga), li)
    qt, th, theta2 = filtered(h)
    ritz[...] = theta2
    ct = mm(qt, li)
    ft = jnp.concatenate(
        [mm(ct[:, :NV], a1t), mm(ct[:, :NV] + ct[:, 2 * NV :], a2t), ct[:, NV : 2 * NV]], axis=1
    )

    for j in range(COLS // CH):
        x, c = divmod(j, NC)
        modes = mm(ft, V[:, j * CH : (j + 1) * CH])
        for y in range(NY):
            for b in range(NV // 8):
                out[pl.ds(b * 384 + (c * NX + x) * NY + y, 8, stride=48), :] = modes[8 * b : 8 * b + 8, tile(y)]

    second[2]()
    third[2]()


def local(sizes, start_block, stiff_field, shift_field, mass_field):
    dofs = 3.0 * stiff_field.size * sizes["gx"] * sizes["gy"] * sizes["gz"]
    rows = NX * NY
    scratch = [
        pltpu.VMEM((3 * NV, COLS), F32),
        pltpu.VMEM((3 * NV, COLS), F32),
        pltpu.VMEM((NV, COLS), F32),
        pltpu.VMEM((NV, COLS), F32),
        pltpu.VMEM((4 * NV, COLS), F32),
        pltpu.VMEM((4 * NV, HALO), F32),
        pltpu.VMEM((2, NV, HALO), F32),
        pltpu.VMEM((8, 2 * CH), F32),
        pltpu.VMEM((2, 8, CH), F32),
        pltpu.VMEM((8, HALO), F32),
        pltpu.VMEM((2, NV, COLS), F32),
        pltpu.VMEM((6, NV + 8, EDGE), F32),
        pltpu.VMEM((2, NV + 8, EDGE), F32),
        pltpu.VMEM((6, NV + 8, T), F32),
        pltpu.VMEM((3, 2, NV + 8, T), F32),
        pltpu.VMEM((3, rows, T), F32),
    ]
    heights = [NV * (i + 1) // 8 for i in range(3)]
    for lead in (8, sizes["gy"], sizes["gx"], sizes["gz"], 8):
        scratch += [pltpu.VMEM((lead, h, T), F32) for h in heights]
    scratch += [pltpu.VMEM((9, NV, NV), F32)]
    scratch += [pltpu.SemaphoreType.DMA((3, 2, 4, 8)), pltpu.SemaphoreType.DMA((3, 2, 8))]
    vmem = pl.BlockSpec(memory_space=pltpu.VMEM)
    modes, ritz = pl.pallas_call(
        functools.partial(kernel, dofs, sizes),
        out_shape=(
            jax.ShapeDtypeStruct((start_block.size // T, T), F32),
            jax.ShapeDtypeStruct((NV, NV), F32),
        ),
        in_specs=[vmem] * 4,
        out_specs=(vmem, vmem),
        scratch_shapes=scratch,
        compiler_params=pltpu.CompilerParams(
            collective_id=0, has_side_effects=True, vmem_limit_bytes=62 * 1024 * 1024
        ),
        name="lobpcg",
    )(
        start_block.reshape(-1, T),
        stiff_field.reshape(rows, T),
        shift_field.reshape(rows, T),
        mass_field.reshape(rows, T),
    )
    return modes.reshape(start_block.shape), ritz


def solution(mesh):
    field = P("gx", "gy", "gz")
    block = P(None, None, "gx", "gy", "gz")
    return jax.shard_map(
        functools.partial(local, dict(mesh.shape)),
        mesh=mesh,
        in_specs=(block, field, field, field),
        out_specs=(block, P()),
        check_vma=False,
    )
```

```python
import functools

import jax
import jax.numpy as jnp
from jax import lax
from jax.experimental import pallas as pl
from jax.experimental.pallas import tpu as pltpu
from jax.sharding import PartitionSpec as P

MESH = pl.DeviceIdType.MESH
F32 = jnp.float32
NV = 64
T = 128
NX, NC, NY = 2, 3, 8
PLANE = NC * NY * T
COLS = NX * PLANE
EDGE = NX * NC * T
X_LO, X_HI = 0, PLANE
Y_LO, Y_HI = 2 * PLANE, 2 * PLANE + EDGE
Z_AT = 2 * PLANE + 2 * EDGE
STEP = 16
HALO = Z_AT + T
CH = NY * T
FAR_FIRST = {4: (2, 1, 3), 8: (4, 3, 5, 2, 6, 1, 7)}


def mm(a, b, ca=1, cb=0):
    return lax.dot_general(
        a, b, (((ca,), (cb,)), ((), ())), precision=lax.Precision.HIGHEST, preferred_element_type=F32
    )


def nt(a, b):
    return mm(a, b, 1, 1)


def tn(a, b):
    return mm(a, b, 0, 0)


def parts_of(x):
    high = x.astype(jnp.bfloat16)
    return high, (x - high.astype(F32)).astype(jnp.bfloat16)


def dot3(a, b, cb=0):
    dims = (((1,), (cb,)), ((), ()))
    small = lax.dot_general(a[1], b[0], dims, preferred_element_type=F32)
    small = small + lax.dot_general(a[0], b[1], dims, preferred_element_type=F32)
    return lax.dot_general(a[0], b[0], dims, preferred_element_type=F32) + small


def eye(n):
    return jnp.where(
        lax.broadcasted_iota(jnp.int32, (n, n), 0) == lax.broadcasted_iota(jnp.int32, (n, n), 1), 1.0, 0.0
    ).astype(F32)


def factor_inverse(a):
    n, p = NV, 8
    m = jnp.concatenate([a, eye(n)], axis=1)

    def full(x):
        return jnp.broadcast_to(x, (8, 2 * n))

    rows = [m[8 * i : 8 * i + 8, :] for i in range(n // 8)]
    sub = lax.broadcasted_iota(jnp.int32, (8, 2 * n), 0)
    pivots = []
    for v in range(n // 8):
        k = v * 8
        col = [{i: full(rows[i][:, k + t : k + t + 1]) for i in range(v, 8)} for t in range(p)]
        blk = [[full(col[u][v][t : t + 1, :]) if u <= t else None for u in range(p)] for t in range(p)]
        row = [full(rows[v][t : t + 1, :]) for t in range(p)]
        fac, piv = [None] * p, [None] * p
        for a_ in range(0, p, 2):
            b_ = a_ + 1
            i0 = 1.0 / blk[a_][a_]
            det = blk[a_][a_] * blk[b_][b_] - blk[b_][a_] * blk[b_][a_]
            i1 = blk[a_][a_] * (1.0 / det)
            low = blk[b_][a_] * i0
            piv[a_] = blk[a_][a_]
            piv[b_] = blk[b_][b_] - low * blk[b_][a_]
            row[b_] = row[b_] - low * row[a_]
            f0 = {i: col[a_][i] * i0 for i in range(v, 8)}
            f1 = {i: (col[b_][i] - col[a_][i] * low) * i1 for i in range(v, 8)}
            fac[a_], fac[b_] = f0, f1
            h0, g1, h1 = {}, {}, {}
            for t in range(b_ + 1, p):
                h0[t] = blk[t][a_] * i0
                g1[t] = blk[t][b_] - h0[t] * blk[b_][a_]
                h1[t] = g1[t] * i1
            for t in range(b_ + 1, p):
                for u in range(b_ + 1, t + 1):
                    blk[t][u] = blk[t][u] - h0[t] * blk[u][a_] - h1[t] * g1[u]
                row[t] = row[t] - h0[t] * row[a_] - h1[t] * row[b_]
                for i in range(v, 8):
                    col[t][i] = col[t][i] - f0[i] * blk[t][a_] - f1[i] * g1[t]
        d = piv[0]
        for t in range(1, p):
            d = jnp.where(sub >= t, piv[t], d)
        pivots.append(d)
        for i in range(v, 8):
            acc = None
            for t in range(p):
                if i == v and t == 7:
                    continue
                f = fac[t][i]
                if i == v:
                    f = jnp.where(sub > t, f, 0.0)
                acc = f * row[t] if acc is None else acc + f * row[t]
            rows[i] = rows[i] - acc
    return jnp.concatenate([r * lax.rsqrt(d) for r, d in zip(rows, pivots)], axis=0)[:, n:]


def filtered(h):
    n = h.shape[0]
    bound = jnp.max(jnp.sum(jnp.abs(h), axis=1, keepdims=True), axis=0, keepdims=True)
    f = eye(n) - h / bound
    f2 = mm(f, f)
    y = mm(f2, f2[:, :NV])
    qt = nt(factor_inverse(tn(y, y)), y)
    th = mm(qt, h)
    return qt, th, nt(th, qt)


def kernel(
    dofs, sizes,
    s, g, e, rho, out, ritz,
    V, VP, KP, H, BP, OP, HB, HS, CF, QX, QH, YP, YK, YR, ZK, ZR,
    P0, P1, P2, A0, A1, A2, B0, B1, B2, C0, C1, C2, D0, D1, D2,
    SM, SQ, SH, ar_sem, halo_sem,
):
    me = {a: lax.axis_index(a) for a in ("gx", "gy", "gz")}
    lane = lax.broadcasted_iota(jnp.int32, (8, T), 1)
    lane_s = lax.broadcasted_iota(jnp.int32, (STEP, T), 1)

    def keep(ref, rows, cols, value):
        ref[0, rows, cols], ref[1, rows, cols] = parts_of(value)

    def peer(axis, off):
        return lax.rem(me[axis] + off, sizes[axis])

    barrier = pltpu.get_barrier_semaphore()
    zero, one = jnp.zeros((NV, NV), F32), eye(NV)
    for axis in ("gx", "gy", "gz"):
        for off in FAR_FIRST[sizes[axis]]:
            pl.semaphore_signal(barrier, inc=1, device_id={axis: peer(axis, off)}, device_id_type=MESH)

    def remote(src, dst, send, recv, axis, to):
        return pltpu.make_async_remote_copy(
            src_ref=src, dst_ref=dst, send_sem=send, recv_sem=recv, device_id={axis: to}, device_id_type=MESH
        )

    def tile(k):
        return slice(k * T, (k + 1) * T)

    def at(x, c, y):
        return (x * NC + c) * NY + y

    def block(start, n=8):
        return pl.ds(pl.multiple_of(start, 8), n)

    diag = 6.0 * g[...] * g[...] + 1.5 * e[...]
    inv = 1.0 / diag
    for i, field in enumerate((g[...], e[...], rho[...], inv, rho[...] * inv, g[...] * inv)):
        for r in range(NX * NY):
            CF[i, :, tile(r)] = jnp.broadcast_to(field[r : r + 1, :], (8, T))
    G_, E_, RHO, INV, Q, GINV = range(6)

    def coef(i, r, n=STEP):
        return jnp.concatenate([CF[i, :, tile(r)]] * (n // 8), axis=0)

    def load(b, _):
        up, down = jnp.zeros((STEP, T), F32), jnp.zeros((STEP, T), F32)
        rows = block(b * STEP, STEP)
        for x in range(NX):
            for y in range(NY):
                r = x * NY + y
                gr, qr, mr = coef(G_, r), coef(Q, r), coef(RHO, r)
                for c in range(NC):
                    k = at(x, c, y)
                    v = s[pl.ds(b * (48 * STEP) + (c * NX + x) * NY + y, STEP, stride=48), :]
                    h = gr * v
                    V[rows, tile(k)] = v
                    keep(VP, rows, tile(k), v)
                    H[rows, tile(k)] = h
                    keep(BP, rows, tile(k), mr * v)
                    keep(OP, block(NV + b * STEP, STEP), tile(k), qr * v)
                    if y == NY - 1:
                        YK[0, rows, tile(x * NC + c)] = h
                    if y == 0:
                        YK[1, rows, tile(x * NC + c)] = h
                    up = jnp.where(lane_s == 2 * k, pltpu.roll(h, (2 * k + 1) % T, 1), up)
                    down = jnp.where(lane_s == (2 * k - 1) % T, pltpu.roll(h, (2 * k - 1) % T, 1), down)
        ZK[0, rows, :] = up
        ZK[1, rows, :] = down
        return 0

    lax.fori_loop(0, NV // STEP, load, 0)
    up, down = jnp.zeros((8, T), F32), jnp.zeros((8, T), F32)
    for x in range(NX):
        for y in range(NY):
            q = CF[Q, :, tile(x * NY + y)]
            for c in range(NC):
                k = at(x, c, y)
                if y == NY - 1:
                    YK[0, NV : NV + 8, tile(x * NC + c)] = q
                if y == 0:
                    YK[1, NV : NV + 8, tile(x * NC + c)] = q
                up = jnp.where(lane == 2 * k, pltpu.roll(q, (2 * k + 1) % T, 1), up)
                down = jnp.where(lane == (2 * k - 1) % T, pltpu.roll(q, (2 * k - 1) % T, 1), down)
    ZK[0, NV : NV + 8, :] = up
    ZK[1, NV : NV + 8, :] = down

    pl.semaphore_wait(barrier, sum(sizes.values()) - 3)

    all_rows = pl.ds(0, NV)

    def exchange(n, faces):
        started, arrived = [], []
        for i, (axis, up_src, down_src, low, high) in enumerate(faces):
            here, size = me[axis], sizes[axis]
            up_copy = remote(
                up_src, low, halo_sem.at[n, 0, 2 * i], halo_sem.at[n, 1, 2 * i], axis, lax.rem(here + 1, size)
            )
            down_copy = remote(
                down_src, high, halo_sem.at[n, 0, 2 * i + 1], halo_sem.at[n, 1, 2 * i + 1],
                axis, lax.rem(here + size - 1, size),
            )
            started += [(here < size - 1, up_copy), (here > 0, down_copy)]
            arrived += [(here > 0, up_copy, low), (here < size - 1, down_copy, high)]

        def start():
            for cond, copy in started:
                pl.when(cond)(copy.start)

        def wait():
            for cond, copy, place in arrived:
                pl.when(cond)(copy.wait_recv)

                @pl.when(jnp.logical_not(cond))
                def _():
                    place[...] = jnp.zeros(place.shape, F32)

        def finish():
            for cond, copy in started:
                pl.when(cond)(copy.wait_send)

        return start, wait, finish

    first = exchange(0, [
        ("gx", H.at[:, PLANE:COLS], H.at[:, 0:PLANE], HS.at[0, :, X_LO : X_LO + PLANE], HS.at[0, :, X_HI : X_HI + PLANE]),
        ("gx", CF.at[Q, :, CH : 2 * CH], CF.at[Q, :, 0:CH], QX.at[0], QX.at[1]),
        ("gy", YK.at[0], YK.at[1], YR.at[0], YR.at[1]),
        ("gz", ZK.at[0], ZK.at[1], ZR.at[0, 0], ZR.at[0, 1]),
    ])

    def later(n):
        top, cut = 2 * NV * (n - 1), 8 * (n + 2)
        row = pl.ds(top, NV)

        def x_faces(a, b):
            mine, theirs = pl.ds(a, b - a), pl.ds(top + a, b - a)
            return (
                "gx", YP.at[n - 1, mine, PLANE:COLS], YP.at[n - 1, mine, 0:PLANE],
                HB.at[theirs, X_LO : X_LO + PLANE], HB.at[theirs, X_HI : X_HI + PLANE],
            )

        early = exchange(3 * n - 2, [x_faces(0, cut)])
        rest = exchange(3 * n - 1, [x_faces(cut, NV)])
        ends = exchange(3 * n, [
            ("gz", ZK.at[2 * n, 0:NV], ZK.at[2 * n + 1, 0:NV], ZR.at[n, 0, 0:NV], ZR.at[n, 1, 0:NV]),
            ("gy", YK.at[2 * n, 0:NV], YK.at[2 * n + 1, 0:NV], HB.at[row, Y_LO : Y_LO + EDGE], HB.at[row, Y_HI : Y_HI + EDGE]),
        ])

        def others():
            rest[0]()
            pack_ends(n - 1)
            ends[0]()

        def every(k):
            for part in (early, ends, rest):
                part[k]()

        return early[0], others, functools.partial(every, 1), functools.partial(every, 2)

    def pack_ends(n):
        def body(b, _):
            rows = block(b * 8)
            up, down = jnp.zeros((8, T), F32), jnp.zeros((8, T), F32)
            for k in range(COLS // T):
                w = YP[n, rows, tile(k)]
                up = jnp.where(lane == 2 * k, pltpu.roll(w, (2 * k + 1) % T, 1), up)
                down = jnp.where(lane == (2 * k - 1) % T, pltpu.roll(w, (2 * k - 1) % T, 1), down)
            ZK[2 * n + 2, rows, :] = up
            ZK[2 * n + 3, rows, :] = down
            return 0

        lax.fori_loop(0, NV // 8, body, 0)

    def stiffness(n, again):
        row = n * NV

        def body(b, _):
            rows, full = block(b * STEP, STEP), block(row + b * STEP, STEP)
            ends = HS[n % 2, rows, Z_AT:HALO]
            held = {}

            def h_at(x, c, y):
                if (x, c, y) not in held:
                    if y < 0:
                        held[x, c, y] = HS[n % 2, rows, Y_LO + (x * NC + c) * T : Y_LO + (x * NC + c + 1) * T]
                    elif y == NY:
                        held[x, c, y] = HS[n % 2, rows, Y_HI + (x * NC + c) * T : Y_HI + (x * NC + c + 1) * T]
                    else:
                        held[x, c, y] = H[rows, tile(at(x, c, y))]
                return held[x, c, y]

            for y in range(NY):
                for x in range(NX):
                    r = x * NY + y
                    gr, er = coef(G_, r), coef(E_, r)
                    vs = [V[rows, tile(at(x, c, y))] for c in range(NC)]
                    half = 0.5 * (vs[0] + vs[1] + vs[2])
                    for c in range(NC):
                        k = at(x, c, y)
                        h = h_at(x, c, y)
                        face = (X_HI if x else X_LO) + (c * NY + y) * T
                        near = h_at(1 - x, c, y) + HS[n % 2, rows, face : face + T]
                        near = near + h_at(x, c, y - 1) + h_at(x, c, y + 1)
                        end = pltpu.roll(ends, (-2 * k) % T, 1) if k else ends
                        near = near + jnp.where(lane_s == 0, end, pltpu.roll(h, 1, 1))
                        near = near + jnp.where(lane_s == T - 1, end, pltpu.roll(h, T - 1, 1))
                        kv = gr * (6.0 * h - near) + er * (vs[c] + half)
                        keep(KP, full, tile(k), kv)
                        if again:
                            keep(OP, block(2 * row + b * STEP, STEP), tile(k), coef(INV, r) * kv)
                            w = coef(GINV, r) * kv
                            YP[n, rows, tile(k)] = w
                            if y == NY - 1:
                                YK[2 * n + 2, rows, tile(x * NC + c)] = w
                            if y == 0:
                                YK[2 * n + 3, rows, tile(x * NC + c)] = w
            return 0

        lax.fori_loop(0, NV // STEP, body, 0)

    def gram(n, mass, part):
        rows = NV * (n + 1)
        left, right, first_row = (VP, BP, 0) if mass else (KP, VP, n * NV)

        def body(j, acc):
            cols = pl.ds(pl.multiple_of(j * CH, CH), CH)
            return acc + dot3(
                [left[i, 0:rows, cols] for i in range(2)],
                [right[i, first_row : first_row + NV, cols] for i in range(2)],
                1,
            )

        total = lax.fori_loop(0, COLS // CH, body, jnp.zeros((rows, NV), F32))
        lanes = slice(0, NV) if mass else slice(NV, 2 * NV)
        part[:, :, lanes] = total.reshape(part.shape[0], part.shape[1], NV)

    def all_reduce(n, part, a, b, c, d, then):
        def spread(phase, axis, source, place):
            here = me[axis]
            copies = []
            for off in FAR_FIRST[sizes[axis]]:
                to = peer(axis, off)
                copy = remote(source(to), place.at[here], ar_sem.at[n, 0, phase, off], ar_sem.at[n, 1, phase, here], axis, to)
                copy.start()
                copies.append(copy)
            return copies

        def collect(phase, axis, place):
            for off in FAR_FIRST[sizes[axis]]:
                frm = peer(axis, off)
                remote(place.at[frm], place.at[frm], ar_sem.at[n, 0, phase, off], ar_sem.at[n, 1, phase, frm], axis, frm).wait_recv()

        def total(place):
            acc = place[0]
            for i in range(1, place.shape[0]):
                acc = acc + place[i]
            return acc

        copies = spread(0, "gy", lambda to: part.at[to], a)
        a[me["gy"]] = part[me["gy"]]
        collect(0, "gy", a)
        b[me["gx"]] = total(a)
        copies += spread(1, "gx", lambda to: b.at[me["gx"]], b)
        collect(1, "gx", b)
        c[me["gz"]] = total(b)
        copies += spread(2, "gz", lambda to: c.at[me["gz"]], c)
        then()
        collect(2, "gz", c)
        d[me["gy"]] = total(c)
        copies += spread(3, "gy", lambda to: d.at[me["gy"]], d)
        collect(3, "gy", d)
        for copy in copies:
            copy.wait_send()
        return d[...].reshape(-1, T) * (1.0 / dofs)

    def residual(n, coeffs):
        depth = 2 * NV * n
        last = n == 2
        own = slice(n * NV, (n + 1) * NV)

        def body(j, _):
            cols = pl.ds(pl.multiple_of(j * CH, CH), CH)
            r = dot3(coeffs, [OP[i, 0:depth, cols] for i in range(2)])
            V[:, cols] = r
            keep(VP, own, cols, r)
            x8 = lax.div(j, NC) * NY
            for y in range(NY):
                part = r[:, tile(y)]
                row = pl.ds(pl.multiple_of((x8 + y) * T, T), T)

                def field(i):
                    return jnp.concatenate([CF[i, :, row]] * (NV // 8), axis=0)

                here = pl.ds(pl.multiple_of(j * CH + y * T, T), T)
                H[:, here] = field(G_) * part
                keep(BP, slice(0, NV), here, field(RHO) * part)
                if not last:
                    keep(OP, slice(depth + NV, depth + 2 * NV), here, field(Q) * part)
            return 0

        lax.fori_loop(0, COLS // CH, body, 0)

    def residual_halo(n, coeffs):
        depth = 2 * NV * n
        last = n == 2

        def put(cols, q):
            r = dot3(coeffs, parts_of(HB[0:depth, cols]))
            HS[n % 2, :, cols] = r
            if not last:
                HB[depth + NV : depth + 2 * NV, cols] = jnp.concatenate([q] * (NV // 8), axis=0) * r

        def body(j, _):
            cols = pl.ds(pl.multiple_of(j * CH, CH), CH)
            put(cols, QH[:, cols])
            return 0

        lax.fori_loop(0, 2 * NC, body, 0)
        put(slice(Y_LO, HALO), QH[:, Y_LO:HALO])

    first[0]()
    gram(0, True, P0)
    first[1]()
    for i, at_x in enumerate((X_LO, X_HI)):
        for c in range(NC):
            QH[:, at_x + c * CH : at_x + (c + 1) * CH] = QX[i]
    for i, at_y in enumerate((Y_LO, Y_HI)):
        HS[0, :, at_y : at_y + EDGE] = YR[i, 0:NV, :]
        QH[:, at_y : at_y + EDGE] = YR[i, NV : NV + 8, :]
    HS[0, :, Z_AT:HALO] = ZR[0, 0, 0:NV, :] + ZR[0, 1, 0:NV, :]
    QH[:, Z_AT:HALO] = ZR[0, 0, NV : NV + 8, :] + ZR[0, 1, NV : NV + 8, :]
    stiffness(0, True)
    second, third = later(1), later(2)
    second[0]()
    gram(0, False, P0)

    def during_first():
        second[1]()
        first[2]()

        def body(b, _):
            for k in range(HALO // T):
                HB[block(NV + b * 8), tile(k)] = QH[:, tile(k)] * HS[0, block(b * 8), tile(k)]
            return 0

        lax.fori_loop(0, NV // 8, body, 0)

    G = all_reduce(0, P0, A0, B0, C0, D0, during_first)
    li0 = factor_inverse(G[:, :NV])
    theta0 = nt(mm(li0, G[:, NV:]), li0)
    c0 = parts_of(jnp.concatenate([li0, -mm(theta0, li0)], axis=1))
    SM[0], SM[1] = li0, theta0
    residual(1, c0)
    gram(1, True, P1)
    second[2]()
    HB[0:NV, Z_AT:HALO] = ZR[1, 0, 0:NV, :] + ZR[1, 1, 0:NV, :]
    residual_halo(1, c0)
    stiffness(1, True)
    third[0]()
    gram(1, False, P1)

    G = all_reduce(1, P1, A1, B1, C1, D1, third[1])
    li0, theta0 = SM[0], SM[1]
    cross = mm(li0, G[:NV, :])
    mxr, kxr = cross[:, :NV], cross[:, NV:]
    li_r = factor_inverse(G[NV:, :NV] - tn(mxr, mxr))
    li = jnp.concatenate(
        [jnp.concatenate([one, zero], axis=1), jnp.concatenate([-nt(li_r, mxr), li_r], axis=1)], axis=0
    )
    ga = jnp.concatenate(
        [jnp.concatenate([theta0, kxr], axis=1), jnp.concatenate([kxr.T, G[NV:, NV:]], axis=1)], axis=0
    )
    h = nt(mm(li, ga), li)
    qt, th, theta1 = filtered(h)
    ct = mm(qt, li)
    a2t = ct[:, NV:]
    a1t = mm(ct[:, :NV], li0)
    c1 = parts_of(jnp.concatenate([a1t, -mm(theta1, a1t), a2t, -mm(theta1, a2t)], axis=1))
    SM[2], SM[3], SM[4], SM[5] = theta1, a1t, a2t, mxr
    SQ[0], SQ[1], SH[...] = qt, th, h
    residual(2, c1)
    gram(2, True, P2)
    third[2]()
    HB[2 * NV : 3 * NV, Z_AT:HALO] = ZR[2, 0, 0:NV, :] + ZR[2, 1, 0:NV, :]
    residual_halo(2, c1)
    stiffness(2, False)
    gram(2, False, P2)

    def during_third():
        qt, th = SQ[0], SQ[1]
        ut = jnp.concatenate([nt(SM[4], SM[5]), qt[:, NV:]], axis=1)
        mxp, mpp = nt(qt, ut), nt(ut, ut)
        SM[6], SM[7], SM[8], SM[9] = mxp, mpp - tn(mxp, mxp), nt(th, ut), nt(mm(ut, SH[...]), ut)

    G = all_reduce(2, P2, A2, B2, C2, D2, during_third)
    theta1, a1t, a2t, _, mxp, spp, kxp, kpp = (SM[i] for i in range(2, 10))
    cross_p = mm(a2t, G[NV : 2 * NV, :])
    cross = mm(jnp.concatenate([a1t, a2t], axis=1), G[: 2 * NV, :])
    mxr, kxr = cross[:, :NV], cross[:, NV:]
    mpr, kpr = cross_p[:, :NV], cross_p[:, NV:]
    li_r = factor_inverse(G[2 * NV :, :NV] - tn(mxr, mxr))
    l32 = nt(mpr - tn(mxp, mxr), li_r)
    li_p = factor_inverse(spp - nt(l32, l32))
    below = -nt(li_r, mxr)
    li = jnp.concatenate(
        [
            jnp.concatenate([one, zero, zero], axis=1),
            jnp.concatenate([below, li_r, zero], axis=1),
            jnp.concatenate([mm(li_p, -mxp.T - mm(l32, below)), -mm(li_p, mm(l32, li_r)), li_p], axis=1),
        ],
        axis=0,
    )
    ga = jnp.concatenate(
        [
            jnp.concatenate([theta1, kxr, kxp], axis=1),
            jnp.concatenate([kxr.T, G[2 * NV :, NV:], kpr.T], axis=1),
            jnp.concatenate([kxp.T, kpr, kpp], axis=1),
        ],
        axis=0,
    )
    h = nt(mm(li, ga), li)
    qt, th, theta2 = filtered(h)
    ritz[...] = theta2
    ct = mm(qt, li)
    ft = parts_of(
        jnp.concatenate(
            [mm(ct[:, :NV], a1t), mm(ct[:, :NV] + ct[:, 2 * NV :], a2t), ct[:, NV : 2 * NV]], axis=1
        )
    )

    for j in range(COLS // CH):
        x, c = divmod(j, NC)
        modes = dot3(ft, [VP[i, :, j * CH : (j + 1) * CH] for i in range(2)])
        for y in range(NY):
            for b in range(NV // 8):
                out[pl.ds(b * 384 + (c * NX + x) * NY + y, 8, stride=48), :] = modes[8 * b : 8 * b + 8, tile(y)]

    second[3]()
    third[3]()


def local(sizes, start_block, stiff_field, shift_field, mass_field):
    dofs = 3.0 * stiff_field.size * sizes["gx"] * sizes["gy"] * sizes["gz"]
    rows = NX * NY
    scratch = [
        pltpu.VMEM((NV, COLS), F32),
        pltpu.VMEM((2, 3 * NV, COLS), jnp.bfloat16),
        pltpu.VMEM((2, 3 * NV, COLS), jnp.bfloat16),
        pltpu.VMEM((NV, COLS), F32),
        pltpu.VMEM((2, NV, COLS), jnp.bfloat16),
        pltpu.VMEM((2, 4 * NV, COLS), jnp.bfloat16),
        pltpu.VMEM((4 * NV, HALO), F32),
        pltpu.VMEM((2, NV, HALO), F32),
        pltpu.VMEM((6, 8, 2 * CH), F32),
        pltpu.VMEM((2, 8, CH), F32),
        pltpu.VMEM((8, HALO), F32),
        pltpu.VMEM((2, NV, COLS), F32),
        pltpu.VMEM((6, NV + 8, EDGE), F32),
        pltpu.VMEM((2, NV + 8, EDGE), F32),
        pltpu.VMEM((6, NV + 8, T), F32),
        pltpu.VMEM((3, 2, NV + 8, T), F32),
    ]
    heights = [NV * (i + 1) // 8 for i in range(3)]
    for lead in (8, sizes["gy"], sizes["gx"], sizes["gz"], 8):
        scratch += [pltpu.VMEM((lead, h, T), F32) for h in heights]
    scratch += [pltpu.VMEM((10, NV, NV), F32)]
    scratch += [pltpu.VMEM((2, NV, 2 * NV), F32), pltpu.VMEM((2 * NV, 2 * NV), F32)]
    scratch += [pltpu.SemaphoreType.DMA((3, 2, 4, 8)), pltpu.SemaphoreType.DMA((7, 2, 8))]
    vmem = pl.BlockSpec(memory_space=pltpu.VMEM)
    modes, ritz = pl.pallas_call(
        functools.partial(kernel, dofs, sizes),
        out_shape=(
            jax.ShapeDtypeStruct((start_block.size // T, T), F32),
            jax.ShapeDtypeStruct((NV, NV), F32),
        ),
        in_specs=[vmem] * 4,
        out_specs=(vmem, vmem),
        scratch_shapes=scratch,
        compiler_params=pltpu.CompilerParams(
            collective_id=0, has_side_effects=True, vmem_limit_bytes=62 * 1024 * 1024
        ),
        name="lobpcg",
    )(
        start_block.reshape(-1, T),
        stiff_field.reshape(rows, T),
        shift_field.reshape(rows, T),
        mass_field.reshape(rows, T),
    )
    return modes.reshape(start_block.shape), ritz


def solution(mesh):
    field = P("gx", "gy", "gz")
    block = P(None, None, "gx", "gy", "gz")
    return jax.shard_map(
        functools.partial(local, dict(mesh.shape)),
        mesh=mesh,
        in_specs=(block, field, field, field),
        out_specs=(block, P()),
        check_vma=False,
    )
```

```python
import functools

import jax
import jax.numpy as jnp
from jax import lax
from jax.experimental import pallas as pl
from jax.experimental.pallas import tpu as pltpu
from jax.sharding import PartitionSpec as P

MESH = pl.DeviceIdType.MESH
F32 = jnp.float32
NV = 64
T = 128
NX, NC, NY = 2, 3, 8
PLANE = NC * NY * T
COLS = NX * PLANE
EDGE = NX * NC * T
X_LO, X_HI = 0, PLANE
Y_LO, Y_HI = 2 * PLANE, 2 * PLANE + EDGE
Z_AT = 2 * PLANE + 2 * EDGE
STEP = 16
HALO = Z_AT + T
CH = NY * T
FAR_FIRST = {4: (2, 1, 3), 8: (4, 3, 5, 2, 6, 1, 7)}


def mm(a, b, ca=1, cb=0):
    return lax.dot_general(
        a, b, (((ca,), (cb,)), ((), ())), precision=lax.Precision.HIGHEST, preferred_element_type=F32
    )


def nt(a, b):
    return mm(a, b, 1, 1)


def tn(a, b):
    return mm(a, b, 0, 0)


def parts_of(x):
    high = x.astype(jnp.bfloat16)
    return high, (x - high.astype(F32)).astype(jnp.bfloat16)


def dot3(a, b, cb=0):
    dims = (((1,), (cb,)), ((), ()))
    small = lax.dot_general(a[1], b[0], dims, preferred_element_type=F32)
    small = small + lax.dot_general(a[0], b[1], dims, preferred_element_type=F32)
    return lax.dot_general(a[0], b[0], dims, preferred_element_type=F32) + small


def eye(n):
    return jnp.where(
        lax.broadcasted_iota(jnp.int32, (n, n), 0) == lax.broadcasted_iota(jnp.int32, (n, n), 1), 1.0, 0.0
    ).astype(F32)


def factor_inverse(a):
    n, p = NV, 8
    m = jnp.concatenate([a, eye(n)], axis=1)

    def full(x):
        return jnp.broadcast_to(x, (8, 2 * n))

    rows = [m[8 * i : 8 * i + 8, :] for i in range(n // 8)]
    sub = lax.broadcasted_iota(jnp.int32, (8, 2 * n), 0)
    pivots = []
    for v in range(n // 8):
        k = v * 8
        col = [{i: full(rows[i][:, k + t : k + t + 1]) for i in range(v, 8)} for t in range(p)]
        blk = [[full(col[u][v][t : t + 1, :]) if u <= t else None for u in range(p)] for t in range(p)]
        row = [full(rows[v][t : t + 1, :]) for t in range(p)]
        fac, piv = [None] * p, [None] * p
        for a_ in range(0, p, 2):
            b_ = a_ + 1
            i0 = 1.0 / blk[a_][a_]
            det = blk[a_][a_] * blk[b_][b_] - blk[b_][a_] * blk[b_][a_]
            i1 = blk[a_][a_] * (1.0 / det)
            low = blk[b_][a_] * i0
            piv[a_] = blk[a_][a_]
            piv[b_] = blk[b_][b_] - low * blk[b_][a_]
            row[b_] = row[b_] - low * row[a_]
            f0 = {i: col[a_][i] * i0 for i in range(v, 8)}
            f1 = {i: (col[b_][i] - col[a_][i] * low) * i1 for i in range(v, 8)}
            fac[a_], fac[b_] = f0, f1
            h0, g1, h1 = {}, {}, {}
            for t in range(b_ + 1, p):
                h0[t] = blk[t][a_] * i0
                g1[t] = blk[t][b_] - h0[t] * blk[b_][a_]
                h1[t] = g1[t] * i1
            for t in range(b_ + 1, p):
                for u in range(b_ + 1, t + 1):
                    blk[t][u] = blk[t][u] - h0[t] * blk[u][a_] - h1[t] * g1[u]
                row[t] = row[t] - h0[t] * row[a_] - h1[t] * row[b_]
                for i in range(v, 8):
                    col[t][i] = col[t][i] - f0[i] * blk[t][a_] - f1[i] * g1[t]
        d = piv[0]
        for t in range(1, p):
            d = jnp.where(sub >= t, piv[t], d)
        pivots.append(d)
        for i in range(v, 8):
            acc = None
            for t in range(p):
                if i == v and t == 7:
                    continue
                f = fac[t][i]
                if i == v:
                    f = jnp.where(sub > t, f, 0.0)
                acc = f * row[t] if acc is None else acc + f * row[t]
            rows[i] = rows[i] - acc
    return jnp.concatenate([r * lax.rsqrt(d) for r, d in zip(rows, pivots)], axis=0)[:, n:]


def filtered(h):
    n = h.shape[0]
    bound = jnp.max(jnp.sum(jnp.abs(h), axis=1, keepdims=True), axis=0, keepdims=True)
    f = eye(n) - h / bound
    f2 = mm(f, f)
    y = mm(f2, f2[:, :NV])
    qt = nt(factor_inverse(tn(y, y)), y)
    th = mm(qt, h)
    return qt, th, nt(th, qt)


def kernel(
    dofs, sizes,
    s, g, e, rho, out, ritz,
    V, VP, KP, H, BP, OP, HB, HS, CF, QX, QH, YP, YK, YR, ZK, ZR,
    *rest,
):
    sums, (SM, SQ, SH, ar_sem, halo_sem) = [rest[i : i + 5] for i in range(0, 30, 5)], rest[30:]
    me = {a: lax.axis_index(a) for a in ("gx", "gy", "gz")}
    lane = lax.broadcasted_iota(jnp.int32, (8, T), 1)
    lane_s = lax.broadcasted_iota(jnp.int32, (STEP, T), 1)

    def keep(ref, rows, cols, value):
        ref[0, rows, cols], ref[1, rows, cols] = parts_of(value)

    def peer(axis, off):
        return lax.rem(me[axis] + off, sizes[axis])

    barrier = pltpu.get_barrier_semaphore()
    zero, one = jnp.zeros((NV, NV), F32), eye(NV)
    for axis in ("gx", "gy", "gz"):
        for off in FAR_FIRST[sizes[axis]]:
            pl.semaphore_signal(barrier, inc=1, device_id={axis: peer(axis, off)}, device_id_type=MESH)

    def remote(src, dst, send, recv, axis, to):
        return pltpu.make_async_remote_copy(
            src_ref=src, dst_ref=dst, send_sem=send, recv_sem=recv, device_id={axis: to}, device_id_type=MESH
        )

    def tile(k):
        return slice(k * T, (k + 1) * T)

    def at(x, c, y):
        return (x * NC + c) * NY + y

    def block(start, n=8):
        return pl.ds(pl.multiple_of(start, 8), n)

    diag = 6.0 * g[...] * g[...] + 1.5 * e[...]
    inv = 1.0 / diag
    for i, field in enumerate((g[...], e[...], rho[...], inv, rho[...] * inv, g[...] * inv)):
        for r in range(NX * NY):
            CF[i, :, tile(r)] = jnp.broadcast_to(field[r : r + 1, :], (8, T))
    G_, E_, RHO, INV, Q, GINV = range(6)

    def coef(i, r, n=STEP):
        return jnp.concatenate([CF[i, :, tile(r)]] * (n // 8), axis=0)

    def load(b, _):
        up, down = jnp.zeros((STEP, T), F32), jnp.zeros((STEP, T), F32)
        rows = block(b * STEP, STEP)
        for x in range(NX):
            for y in range(NY):
                r = x * NY + y
                gr, qr, mr = coef(G_, r), coef(Q, r), coef(RHO, r)
                for c in range(NC):
                    k = at(x, c, y)
                    v = s[pl.ds(b * (48 * STEP) + (c * NX + x) * NY + y, STEP, stride=48), :]
                    h = gr * v
                    V[rows, tile(k)] = v
                    keep(VP, rows, tile(k), v)
                    H[rows, tile(k)] = h
                    keep(BP, rows, tile(k), mr * v)
                    keep(OP, block(NV + b * STEP, STEP), tile(k), qr * v)
                    if y == NY - 1:
                        YK[0, rows, tile(x * NC + c)] = h
                    if y == 0:
                        YK[1, rows, tile(x * NC + c)] = h
                    up = jnp.where(lane_s == 2 * k, pltpu.roll(h, (2 * k + 1) % T, 1), up)
                    down = jnp.where(lane_s == (2 * k - 1) % T, pltpu.roll(h, (2 * k - 1) % T, 1), down)
        ZK[0, rows, :] = up
        ZK[1, rows, :] = down
        return 0

    lax.fori_loop(0, NV // STEP, load, 0)
    up, down = jnp.zeros((8, T), F32), jnp.zeros((8, T), F32)
    for x in range(NX):
        for y in range(NY):
            q = CF[Q, :, tile(x * NY + y)]
            for c in range(NC):
                k = at(x, c, y)
                if y == NY - 1:
                    YK[0, NV : NV + 8, tile(x * NC + c)] = q
                if y == 0:
                    YK[1, NV : NV + 8, tile(x * NC + c)] = q
                up = jnp.where(lane == 2 * k, pltpu.roll(q, (2 * k + 1) % T, 1), up)
                down = jnp.where(lane == (2 * k - 1) % T, pltpu.roll(q, (2 * k - 1) % T, 1), down)
    ZK[0, NV : NV + 8, :] = up
    ZK[1, NV : NV + 8, :] = down

    pl.semaphore_wait(barrier, sum(sizes.values()) - 3)

    all_rows = pl.ds(0, NV)

    def exchange(n, faces):
        started, arrived = [], []
        for i, (axis, up_src, down_src, low, high) in enumerate(faces):
            here, size = me[axis], sizes[axis]
            up_copy = remote(
                up_src, low, halo_sem.at[n, 0, 2 * i], halo_sem.at[n, 1, 2 * i], axis, lax.rem(here + 1, size)
            )
            down_copy = remote(
                down_src, high, halo_sem.at[n, 0, 2 * i + 1], halo_sem.at[n, 1, 2 * i + 1],
                axis, lax.rem(here + size - 1, size),
            )
            started += [(here < size - 1, up_copy), (here > 0, down_copy)]
            arrived += [(here > 0, up_copy, low), (here < size - 1, down_copy, high)]

        def start():
            for cond, copy in started:
                pl.when(cond)(copy.start)

        def wait():
            for cond, copy, place in arrived:
                pl.when(cond)(copy.wait_recv)

                @pl.when(jnp.logical_not(cond))
                def _():
                    place[...] = jnp.zeros(place.shape, F32)

        def finish():
            for cond, copy in started:
                pl.when(cond)(copy.wait_send)

        return start, wait, finish

    first = exchange(0, [
        ("gx", H.at[:, PLANE:COLS], H.at[:, 0:PLANE], HS.at[0, :, X_LO : X_LO + PLANE], HS.at[0, :, X_HI : X_HI + PLANE]),
        ("gx", CF.at[Q, :, CH : 2 * CH], CF.at[Q, :, 0:CH], QX.at[0], QX.at[1]),
        ("gy", YK.at[0], YK.at[1], YR.at[0], YR.at[1]),
        ("gz", ZK.at[0], ZK.at[1], ZR.at[0, 0], ZR.at[0, 1]),
    ])

    def later(n):
        top, cut = 2 * NV * (n - 1), 8 * (n + 1)
        row = pl.ds(top, NV)

        def x_faces(a, b):
            mine, theirs = pl.ds(a, b - a), pl.ds(top + a, b - a)
            return (
                "gx", YP.at[n - 1, mine, PLANE:COLS], YP.at[n - 1, mine, 0:PLANE],
                HB.at[theirs, X_LO : X_LO + PLANE], HB.at[theirs, X_HI : X_HI + PLANE],
            )

        early = exchange(3 * n - 2, [x_faces(0, cut)])
        rest = exchange(3 * n - 1, [x_faces(cut, NV)])
        ends = exchange(3 * n, [
            ("gz", ZK.at[2 * n, 0:NV], ZK.at[2 * n + 1, 0:NV], ZR.at[n, 0, 0:NV], ZR.at[n, 1, 0:NV]),
            ("gy", YK.at[2 * n, 0:NV], YK.at[2 * n + 1, 0:NV], HB.at[row, Y_LO : Y_LO + EDGE], HB.at[row, Y_HI : Y_HI + EDGE]),
        ])

        def others():
            rest[0]()
            pack_ends(n - 1)
            ends[0]()

        def every(k):
            for part in (early, ends, rest):
                part[k]()

        return early[0], others, functools.partial(every, 1), functools.partial(every, 2)

    def pack_ends(n):
        def body(b, _):
            rows = block(b * 8)
            up, down = jnp.zeros((8, T), F32), jnp.zeros((8, T), F32)
            for k in range(COLS // T):
                w = YP[n, rows, tile(k)]
                up = jnp.where(lane == 2 * k, pltpu.roll(w, (2 * k + 1) % T, 1), up)
                down = jnp.where(lane == (2 * k - 1) % T, pltpu.roll(w, (2 * k - 1) % T, 1), down)
            ZK[2 * n + 2, rows, :] = up
            ZK[2 * n + 3, rows, :] = down
            return 0

        lax.fori_loop(0, NV // 8, body, 0)

    def stiffness(n, again):
        row = n * NV

        def body(b, _):
            rows, full = block(b * STEP, STEP), block(row + b * STEP, STEP)
            ends = HS[n % 2, rows, Z_AT:HALO]
            held = {}

            def h_at(x, c, y):
                if (x, c, y) not in held:
                    if y < 0:
                        held[x, c, y] = HS[n % 2, rows, Y_LO + (x * NC + c) * T : Y_LO + (x * NC + c + 1) * T]
                    elif y == NY:
                        held[x, c, y] = HS[n % 2, rows, Y_HI + (x * NC + c) * T : Y_HI + (x * NC + c + 1) * T]
                    else:
                        held[x, c, y] = H[rows, tile(at(x, c, y))]
                return held[x, c, y]

            for y in range(NY):
                for x in range(NX):
                    r = x * NY + y
                    gr, er = coef(G_, r), coef(E_, r)
                    vs = [V[rows, tile(at(x, c, y))] for c in range(NC)]
                    half = 0.5 * (vs[0] + vs[1] + vs[2])
                    for c in range(NC):
                        k = at(x, c, y)
                        h = h_at(x, c, y)
                        face = (X_HI if x else X_LO) + (c * NY + y) * T
                        near = h_at(1 - x, c, y) + HS[n % 2, rows, face : face + T]
                        near = near + h_at(x, c, y - 1) + h_at(x, c, y + 1)
                        end = pltpu.roll(ends, (-2 * k) % T, 1) if k else ends
                        near = near + jnp.where(lane_s == 0, end, pltpu.roll(h, 1, 1))
                        near = near + jnp.where(lane_s == T - 1, end, pltpu.roll(h, T - 1, 1))
                        kv = gr * (6.0 * h - near) + er * (vs[c] + half)
                        keep(KP, full, tile(k), kv)
                        if again:
                            keep(OP, block(2 * row + b * STEP, STEP), tile(k), coef(INV, r) * kv)
                            w = coef(GINV, r) * kv
                            YP[n, rows, tile(k)] = w
                            if y == NY - 1:
                                YK[2 * n + 2, rows, tile(x * NC + c)] = w
                            if y == 0:
                                YK[2 * n + 3, rows, tile(x * NC + c)] = w
            return 0

        lax.fori_loop(0, NV // STEP, body, 0)

    def gram(n, mass, part):
        rows = NV * (n + 1)
        left, right, first_row = (VP, BP, 0) if mass else (KP, VP, n * NV)

        def body(j, acc):
            cols = pl.ds(pl.multiple_of(j * CH, CH), CH)
            big, small = left[0, 0:rows, cols], left[1, 0:rows, cols]
            pair = [right[i, first_row : first_row + NV, cols] for i in range(2)]
            dims = (((1,), (1,)), ((), ()))
            both = lax.dot_general(jnp.concatenate([big, small], axis=0), pair[0], dims, preferred_element_type=F32)
            last = lax.dot_general(big, pair[1], dims, preferred_element_type=F32)
            return acc + both[:rows] + (both[rows:] + last)

        total = lax.fori_loop(0, COLS // CH, body, jnp.zeros((rows, NV), F32))
        part[...] = jnp.concatenate([total, total], axis=1).reshape(part.shape)

    def reducer(n):
        part, a, b, c, d = sums[n]
        copies = []

        def spread(phase, axis, source, place):
            here = me[axis]
            copies = []
            for off in FAR_FIRST[sizes[axis]]:
                to = peer(axis, off)
                copy = remote(source(to), place.at[here], ar_sem.at[n, 0, phase, off], ar_sem.at[n, 1, phase, here], axis, to)
                copy.start()
                copies.append(copy)
            return copies

        def collect(phase, axis, place):
            for off in FAR_FIRST[sizes[axis]]:
                frm = peer(axis, off)
                remote(place.at[frm], place.at[frm], ar_sem.at[n, 0, phase, off], ar_sem.at[n, 1, phase, frm], axis, frm).wait_recv()

        def total(place):
            acc = place[0]
            for i in range(1, place.shape[0]):
                acc = acc + place[i]
            return acc

        def step0():
            copies.extend(spread(0, "gy", lambda to: part.at[to], a))
            a[me["gy"]] = part[me["gy"]]

        def step1():
            collect(0, "gy", a)
            b[me["gx"]] = total(a)
            copies.extend(spread(1, "gx", lambda to: b.at[me["gx"]], b))

        def step2():
            collect(1, "gx", b)
            c[me["gz"]] = total(b)
            copies.extend(spread(2, "gz", lambda to: c.at[me["gz"]], c))

        def step3():
            collect(2, "gz", c)
            d[me["gy"]] = total(c)
            copies.extend(spread(3, "gy", lambda to: d.at[me["gy"]], d))

        def step4():
            collect(3, "gy", d)
            for copy in copies:
                copy.wait_send()
            return d[...].reshape(-1, T)[:, :NV] * (1.0 / dofs)

        return step0, step1, step2, step3, step4

    def residual(n, coeffs):
        depth = 2 * NV * n
        last = n == 2
        own = slice(n * NV, (n + 1) * NV)

        def body(j, _):
            cols = pl.ds(pl.multiple_of(j * CH, CH), CH)
            r = dot3(coeffs, [OP[i, 0:depth, cols] for i in range(2)])
            V[:, cols] = r
            keep(VP, own, cols, r)
            x8 = lax.div(j, NC) * NY
            for y in range(NY):
                part = r[:, tile(y)]
                row = pl.ds(pl.multiple_of((x8 + y) * T, T), T)

                def field(i):
                    return jnp.concatenate([CF[i, :, row]] * (NV // 8), axis=0)

                here = pl.ds(pl.multiple_of(j * CH + y * T, T), T)
                H[:, here] = field(G_) * part
                keep(BP, slice(0, NV), here, field(RHO) * part)
                if not last:
                    keep(OP, slice(depth + NV, depth + 2 * NV), here, field(Q) * part)
            return 0

        lax.fori_loop(0, COLS // CH, body, 0)

    def residual_halo(n, coeffs):
        depth = 2 * NV * n
        last = n == 2

        def put(cols, q):
            r = dot3(coeffs, parts_of(HB[0:depth, cols]))
            HS[n % 2, :, cols] = r
            if not last:
                HB[depth + NV : depth + 2 * NV, cols] = jnp.concatenate([q] * (NV // 8), axis=0) * r

        def body(j, _):
            cols = pl.ds(pl.multiple_of(j * CH, CH), CH)
            put(cols, QH[:, cols])
            return 0

        lax.fori_loop(0, 2 * NC, body, 0)
        put(slice(Y_LO, HALO), QH[:, Y_LO:HALO])

    mass = [reducer(n) for n in range(3)]
    stiff = [reducer(n + 3) for n in range(3)]
    first[0]()
    gram(0, True, sums[0][0])
    mass[0][0]()
    first[1]()
    mass[0][1]()
    for i, at_x in enumerate((X_LO, X_HI)):
        for c in range(NC):
            QH[:, at_x + c * CH : at_x + (c + 1) * CH] = QX[i]
    for i, at_y in enumerate((Y_LO, Y_HI)):
        HS[0, :, at_y : at_y + EDGE] = YR[i, 0:NV, :]
        QH[:, at_y : at_y + EDGE] = YR[i, NV : NV + 8, :]
    HS[0, :, Z_AT:HALO] = ZR[0, 0, 0:NV, :] + ZR[0, 1, 0:NV, :]
    QH[:, Z_AT:HALO] = ZR[0, 0, NV : NV + 8, :] + ZR[0, 1, NV : NV + 8, :]
    stiffness(0, True)
    second, third = later(1), later(2)
    second[0]()
    gram(0, False, sums[3][0])
    mass[0][2]()
    stiff[0][0]()
    mass[0][3]()
    stiff[0][1]()
    stiff[0][2]()
    second[1]()
    first[2]()

    def scale(b, _):
        for k in range(HALO // T):
            HB[block(NV + b * 8), tile(k)] = QH[:, tile(k)] * HS[0, block(b * 8), tile(k)]
        return 0

    lax.fori_loop(0, NV // 8, scale, 0)
    gm = mass[0][4]()
    stiff[0][3]()
    SM[0] = factor_inverse(gm)
    gk = stiff[0][4]()
    li0 = SM[0]
    theta0 = nt(mm(li0, gk), li0)
    c0 = parts_of(jnp.concatenate([li0, -mm(theta0, li0)], axis=1))
    SM[1] = theta0
    residual(1, c0)
    gram(1, True, sums[1][0])
    mass[1][0]()
    second[2]()
    HB[0:NV, Z_AT:HALO] = ZR[1, 0, 0:NV, :] + ZR[1, 1, 0:NV, :]
    residual_halo(1, c0)
    mass[1][1]()
    stiffness(1, True)
    third[0]()
    gram(1, False, sums[4][0])

    mass[1][2]()
    stiff[1][0]()
    mass[1][3]()
    stiff[1][1]()
    stiff[1][2]()
    third[1]()
    gm = mass[1][4]()
    stiff[1][3]()
    mxr = mm(SM[0], gm[:NV, :])
    li_r = factor_inverse(gm[NV:, :] - tn(mxr, mxr))
    SM[5], SM[10], SM[11] = mxr, li_r, -nt(li_r, mxr)
    gk = stiff[1][4]()
    li0, theta0 = SM[0], SM[1]
    kxr = mm(li0, gk[:NV, :])
    li = jnp.concatenate(
        [jnp.concatenate([one, zero], axis=1), jnp.concatenate([SM[11], SM[10]], axis=1)], axis=0
    )
    ga = jnp.concatenate(
        [jnp.concatenate([theta0, kxr], axis=1), jnp.concatenate([kxr.T, gk[NV:, :]], axis=1)], axis=0
    )
    h = nt(mm(li, ga), li)
    qt, th, theta1 = filtered(h)
    ct = mm(qt, li)
    a2t = ct[:, NV:]
    a1t = mm(ct[:, :NV], li0)
    c1 = parts_of(jnp.concatenate([a1t, -mm(theta1, a1t), a2t, -mm(theta1, a2t)], axis=1))
    SM[2], SM[3], SM[4] = theta1, a1t, a2t
    SQ[0], SQ[1], SH[...] = qt, th, h
    residual(2, c1)
    gram(2, True, sums[2][0])
    mass[2][0]()
    qt, th = SQ[0], SQ[1]
    ut = jnp.concatenate([nt(SM[4], SM[5]), qt[:, NV:]], axis=1)
    mxp, mpp = nt(qt, ut), nt(ut, ut)
    SM[6], SM[7], SM[8], SM[9] = mxp, mpp - tn(mxp, mxp), nt(th, ut), nt(mm(ut, SH[...]), ut)
    third[2]()
    HB[2 * NV : 3 * NV, Z_AT:HALO] = ZR[2, 0, 0:NV, :] + ZR[2, 1, 0:NV, :]
    residual_halo(2, c1)
    mass[2][1]()
    stiffness(2, False)
    gram(2, False, sums[5][0])

    mass[2][2]()
    stiff[2][0]()
    stiff[2][1]()
    mass[2][3]()
    stiff[2][2]()
    gm = mass[2][4]()
    stiff[2][3]()
    both = jnp.concatenate([SM[3], SM[4]], axis=1)
    mxr = mm(both, gm[: 2 * NV, :])
    mpr = mm(SM[4], gm[NV : 2 * NV, :])
    mxp = SM[6]
    li_r = factor_inverse(gm[2 * NV :, :] - tn(mxr, mxr))
    l32 = nt(mpr - tn(mxp, mxr), li_r)
    li_p = factor_inverse(SM[7] - nt(l32, l32))
    below = -nt(li_r, mxr)
    SM[10], SM[11], SM[12] = li_r, below, li_p
    SM[13], SM[14] = mm(li_p, -mxp.T - mm(l32, below)), -mm(li_p, mm(l32, li_r))
    gk = stiff[2][4]()
    theta1, a1t, a2t, kxp, kpp = SM[2], SM[3], SM[4], SM[8], SM[9]
    kxr = mm(jnp.concatenate([a1t, a2t], axis=1), gk[: 2 * NV, :])
    kpr = mm(a2t, gk[NV : 2 * NV, :])
    li = jnp.concatenate(
        [
            jnp.concatenate([one, zero, zero], axis=1),
            jnp.concatenate([SM[11], SM[10], zero], axis=1),
            jnp.concatenate([SM[13], SM[14], SM[12]], axis=1),
        ],
        axis=0,
    )
    ga = jnp.concatenate(
        [
            jnp.concatenate([theta1, kxr, kxp], axis=1),
            jnp.concatenate([kxr.T, gk[2 * NV :, :], kpr.T], axis=1),
            jnp.concatenate([kxp.T, kpr, kpp], axis=1),
        ],
        axis=0,
    )
    h = nt(mm(li, ga), li)
    qt, th, theta2 = filtered(h)
    ritz[...] = theta2
    ct = mm(qt, li)
    ft = parts_of(
        jnp.concatenate(
            [mm(ct[:, :NV], a1t), mm(ct[:, :NV] + ct[:, 2 * NV :], a2t), ct[:, NV : 2 * NV]], axis=1
        )
    )

    for j in range(COLS // CH):
        x, c = divmod(j, NC)
        modes = dot3(ft, [VP[i, :, j * CH : (j + 1) * CH] for i in range(2)])
        for y in range(NY):
            for b in range(NV // 8):
                out[pl.ds(b * 384 + (c * NX + x) * NY + y, 8, stride=48), :] = modes[8 * b : 8 * b + 8, tile(y)]

    second[3]()
    third[3]()


def local(sizes, start_block, stiff_field, shift_field, mass_field):
    dofs = 3.0 * stiff_field.size * sizes["gx"] * sizes["gy"] * sizes["gz"]
    rows = NX * NY
    scratch = [
        pltpu.VMEM((NV, COLS), F32),
        pltpu.VMEM((2, 3 * NV, COLS), jnp.bfloat16),
        pltpu.VMEM((2, 3 * NV, COLS), jnp.bfloat16),
        pltpu.VMEM((NV, COLS), F32),
        pltpu.VMEM((2, NV, COLS), jnp.bfloat16),
        pltpu.VMEM((2, 4 * NV, COLS), jnp.bfloat16),
        pltpu.VMEM((4 * NV, HALO), F32),
        pltpu.VMEM((2, NV, HALO), F32),
        pltpu.VMEM((6, 8, 2 * CH), F32),
        pltpu.VMEM((2, 8, CH), F32),
        pltpu.VMEM((8, HALO), F32),
        pltpu.VMEM((2, NV, COLS), F32),
        pltpu.VMEM((6, NV + 8, EDGE), F32),
        pltpu.VMEM((2, NV + 8, EDGE), F32),
        pltpu.VMEM((6, NV + 8, T), F32),
        pltpu.VMEM((3, 2, NV + 8, T), F32),
    ]
    heights = [NV * (i + 1) // 8 for i in range(3)]
    for height in 2 * heights:
        scratch += [pltpu.VMEM((lead, height, T), F32) for lead in (8, sizes["gy"], sizes["gx"], sizes["gz"], 8)]
    scratch += [pltpu.VMEM((15, NV, NV), F32)]
    scratch += [pltpu.VMEM((2, NV, 2 * NV), F32), pltpu.VMEM((2 * NV, 2 * NV), F32)]
    scratch += [pltpu.SemaphoreType.DMA((6, 2, 4, 8)), pltpu.SemaphoreType.DMA((7, 2, 8))]
    vmem = pl.BlockSpec(memory_space=pltpu.VMEM)
    modes, ritz = pl.pallas_call(
        functools.partial(kernel, dofs, sizes),
        out_shape=(
            jax.ShapeDtypeStruct((start_block.size // T, T), F32),
            jax.ShapeDtypeStruct((NV, NV), F32),
        ),
        in_specs=[vmem] * 4,
        out_specs=(vmem, vmem),
        scratch_shapes=scratch,
        compiler_params=pltpu.CompilerParams(
            collective_id=0, has_side_effects=True, vmem_limit_bytes=62 * 1024 * 1024
        ),
        name="lobpcg",
    )(
        start_block.reshape(-1, T),
        stiff_field.reshape(rows, T),
        shift_field.reshape(rows, T),
        mass_field.reshape(rows, T),
    )
    return modes.reshape(start_block.shape), ritz


def solution(mesh):
    field = P("gx", "gy", "gz")
    block = P(None, None, "gx", "gy", "gz")
    return jax.shard_map(
        functools.partial(local, dict(mesh.shape)),
        mesh=mesh,
        in_specs=(block, field, field, field),
        out_specs=(block, P()),
        check_vma=False,
    )
```
